32 devices in a mesh: chan: 4 (over y, x), slab: 8 (over z, core).
Axes of the slice: x: 2, y: 2, z: 4, core: 2. Of those that a mesh axis runs over, the one named last changes fastest.
Arguments:
- taylor_models: float32 [2, 2048, 2048], P(None, 'slab', 'chan'), may hold values from -6 to 6
- gridded_vis: bfloat16 [4, 2, 2048, 2048], P('chan', None, 'slab'), may hold values from -6 to 6
- uv_weight: bfloat16 [4, 2048, 2048], P('chan', 'slab'), may hold values from 0 to 2
- freq_ratio: float32 [4], P('chan'), may hold values from 0.6 to 1.4
- robust_scale: float32 [4], P('chan'), may hold values from 0.25 to 4
Outputs:
- taylor_residual: float32 [2, 2048, 2048], P(None, 'slab', 'chan')
The draws below stay inside these ranges and needn't reach their ends.
All inputs are finite; a program needn't handle non-finite values.
Results may differ from the reference program's by a relative error of at most 0.0003.
Values sent between devices are 32-bit elements; how exact they have to be, the bound alone decides.
No kernel may reach another device: no remote copies, remote signals or barrier semaphores. Data moves between devices by JAX's collectives and lax.ppermute only.
A program may use at most 64 MiB of HBM per device.

```python
import math
import jax
import jax.numpy as jnp
from jax import lax

PIX = 2048
TERMS = 2
CHANNELS = 4


def levels(key, dims, cuts, smallest, largest):
    factor_of = 1.0
    for position, parts in cuts:
        steps = jax.random.uniform(jax.random.fold_in(jax.random.fold_in(key, 6), position), (parts,), jnp.float32, smallest / len(cuts), largest / len(cuts))
        factor_of = factor_of * jnp.repeat(jnp.exp(steps), dims[position] // parts).reshape((-1,) + (1,) * (len(dims) - 1 - position))
    return factor_of


def centred(own_key, extent, deviation, bound, pieces=(), dtype=jnp.bfloat16):
    entries = deviation * jax.random.normal(own_key, extent, jnp.float32)
    if pieces:
        entries = entries * levels(own_key, extent, pieces, -0.22, 0.18)
    return jnp.clip(entries, -bound, bound).astype(dtype)


def setup_inputs(seed: int = 0) -> dict:
    keys = jax.random.split(jax.random.key(seed), 6)
    taylor_models = centred(keys[0], (TERMS, PIX, PIX), 1.0, 6.0, ((1, 8), (2, 4)), jnp.float32)
    gridded_vis = centred(keys[1], (CHANNELS, 2, PIX, PIX), 1.0, 6.0, ((0, 4), (2, 8)))
    uv_weight = jnp.clip(2.0 * jax.random.uniform(keys[2], (CHANNELS, PIX, PIX), jnp.float32) ** levels(keys[2], (CHANNELS, PIX, PIX), ((0, 4), (1, 8)), -0.2, 0.2), 0.0, 2.0).astype(jnp.bfloat16)
    freq_ratio = jnp.clip(0.6 + 0.79999995 * jax.random.uniform(keys[3], (CHANNELS,), jnp.float32) ** levels(keys[3], (CHANNELS,), ((0, 4),), -0.2, 0.2), 0.6, 1.4)
    robust_scale = jnp.clip(jnp.exp(math.log(4.0) - 2.7725887 * jax.random.uniform(keys[4], (CHANNELS,), jnp.float32) ** levels(keys[4], (CHANNELS,), ((0, 4),), -0.2, 0.2)), 0.25, 4.0)
    return {"taylor_models": taylor_models, "gridded_vis": gridded_vis, "uv_weight": uv_weight, "freq_ratio": freq_ratio, "robust_scale": robust_scale}


def reference(taylor_models, gridded_vis, uv_weight, freq_ratio, robust_scale):
    def one_channel(carry, item):
        visible, weight, ratio, damping = item
        offset = ratio - 1.0
        sky_image = taylor_models[0]
        for term_index in range(1, TERMS):
            sky_image = sky_image + offset ** term_index * taylor_models[term_index]
        spectrum = jnp.fft.fft2(sky_image, norm="ortho").T
        visible_wide = visible.astype(jnp.float32)
        weight_wide = weight.astype(jnp.float32)
        delta_real = visible_wide[0] - weight_wide * jnp.real(spectrum)
        delta_imag = visible_wide[1] - weight_wide * jnp.imag(spectrum)
        robust = 1.0 / (1.0 + damping * (delta_real * delta_real + delta_imag * delta_imag))
        weighted = lax.complex(robust * delta_real, robust * delta_imag)
        residual = jnp.real(jnp.fft.ifft2(weighted.T, norm="ortho"))
        layers = [residual]
        for term_index in range(1, TERMS):
            layers.append(offset ** term_index * residual)
        return carry + jnp.stack(layers), None

    initial = jnp.zeros((TERMS, PIX, PIX), jnp.float32)
    total, _ = lax.scan(one_channel, initial, (gridded_vis, uv_weight, freq_ratio, robust_scale))
    return total
```

```python
import functools
import math

import jax
import jax.numpy as jnp
import numpy as np
from jax import lax
from jax.experimental import pallas as pl
from jax.experimental.pallas import tpu as pltpu
from jax.sharding import PartitionSpec as P

INNER = 128


def split_bf16(x):
    high = x.astype(jnp.bfloat16)
    low = (x - high.astype(jnp.float32)).astype(jnp.bfloat16)
    return high, low


def table_pair(table):
    high = table.astype(np.float32).astype(jnp.bfloat16)
    low = (table - high.astype(np.float64)).astype(np.float32).astype(jnp.bfloat16)
    return np.stack([high, low])


@functools.cache
def tables(points):
    outer = points // INNER
    steps = np.arange(INNER)
    angle = 2.0 * np.pi * (np.outer(steps, steps) % INNER) / INNER
    cos, sin = np.cos(angle), np.sin(angle)
    forward = np.block([[cos, -sin], [sin, cos]])
    inverse = np.block([[cos, sin], [-sin, cos]])
    twist = 2.0 * np.pi * np.outer(np.arange(outer), steps) / points
    twist_table = np.stack([np.cos(twist), np.sin(twist)]).astype(np.float32)
    return table_pair(forward), table_pair(inverse), twist_table


def plus(x, y):
    return y if x is None else x if y is None else x + y


def minus(x, y):
    if y is None:
        return x
    return -y if x is None else x - y


def short_dft(values, sign):
    count = len(values)
    if count == 1:
        return values
    even = short_dft(values[0::2], sign)
    odd = short_dft(values[1::2], sign)
    half = count // 2
    out = [None] * count
    for k in range(half):
        (er, ei), (orr, oi) = even[k], odd[k]
        if k == 0:
            tr, ti = orr, oi
        elif 4 * k == count:
            tr, ti = (minus(None, oi), orr) if sign > 0 else (oi, minus(None, orr))
        else:
            c = math.cos(2.0 * math.pi * k / count)
            s = sign * math.sin(2.0 * math.pi * k / count)
            tr = minus(orr * c, None if oi is None else oi * s)
            ti = plus(orr * s, None if oi is None else oi * c)
        out[k] = (plus(er, tr), plus(ei, ti))
        out[k + half] = (minus(er, tr), minus(ei, ti))
    return out


def triple_dot(x, table_ref):
    high, low = split_bf16(x)
    dot = functools.partial(jnp.dot, preferred_element_type=jnp.float32)
    return dot(high, table_ref[0]) + dot(low, table_ref[0]) + dot(high, table_ref[1])


def rows_forward(x_ref, table_ref, twist_ref, out_ref):
    blocks, rows, width = x_ref.shape
    outer = blocks * width // INNER
    pieces = []
    for block in range(blocks):
        for start in range(0, width, INNER):
            pieces.append((x_ref[block, :, start : start + INNER], None))
    parts = short_dft(pieces, -1)
    turned = []
    for j in range(outer):
        re, im = parts[j]
        if im is None:
            im = jnp.zeros_like(re)
        c, s = twist_ref[0, j : j + 1, :], twist_ref[1, j : j + 1, :]
        turned.append(jnp.concatenate([re * c + im * s, im * c - re * s], axis=1))
    done = triple_dot(jnp.concatenate(turned, axis=0), table_ref)
    for j in range(outer):
        flipped = done[j * rows : (j + 1) * rows].T
        out_ref[0, j] = flipped[:INNER]
        out_ref[1, j] = flipped[INNER:]


def rows_inverse(x_ref, table_ref, twist_ref, out_ref):
    blocks, rows, width = out_ref.shape
    outer = x_ref.shape[1]
    scale = 1.0 / (outer * INNER)
    lines = [
        jnp.concatenate([x_ref[0, j], x_ref[1, j]], axis=0).T for j in range(outer)
    ]
    done = triple_dot(jnp.concatenate(lines, axis=0), table_ref)
    turned = []
    for j in range(outer):
        part = done[j * rows : (j + 1) * rows]
        re, im = part[:, :INNER], part[:, INNER:]
        c, s = twist_ref[0, j : j + 1, :] * scale, twist_ref[1, j : j + 1, :] * scale
        turned.append((re * c - im * s, im * c + re * s))
    result = short_dft(turned, 1)
    per_block = width // INNER
    for b in range(outer):
        start = (b % per_block) * INNER
        out_ref[b // per_block, :, start : start + INNER] = result[b][0]


def middle(
    damping_ref, x_ref, vis_ref, weight_ref, ahead_ref, back_ref, twist_ref, out_ref, work_ref, wide_ref
):
    _, outer, rows, _ = x_ref.shape
    scale = 1.0 / (outer * INNER)
    joined = jnp.concatenate(
        [x_ref[0].reshape(outer * rows, INNER), x_ref[1].reshape(outer * rows, INNER)], axis=1
    )
    work_ref[...] = triple_dot(joined, ahead_ref).reshape(outer, rows, 2 * INNER)
    wide_ref[0] = vis_ref[0, 0].astype(jnp.float32)
    wide_ref[1] = vis_ref[0, 1].astype(jnp.float32)
    wide_ref[2] = weight_ref[0].astype(jnp.float32)
    damping = damping_ref[0]

    def step(index, carry):
        at = pl.ds(pl.multiple_of(index * 8, 8), 8)
        values = []
        for b in range(outer):
            re, im = work_ref[b, at, :INNER], work_ref[b, at, INNER:]
            c, s = twist_ref[0, b : b + 1, :] * scale, twist_ref[1, b : b + 1, :] * scale
            values.append((re * c + im * s, im * c - re * s))
        spectrum = short_dft(values, -1)
        weighted = []
        for j in range(outer):
            lanes = slice(j * INNER, (j + 1) * INNER)
            weight = wide_ref[2, at, lanes]
            re = wide_ref[0, at, lanes] - weight * spectrum[j][0]
            im = wide_ref[1, at, lanes] - weight * spectrum[j][1]
            robust = 1.0 / (1.0 + damping * (re * re + im * im))
            weighted.append((robust * re, robust * im))
        inverse = short_dft(weighted, 1)
        for b in range(outer):
            re, im = inverse[b]
            c, s = twist_ref[0, b : b + 1, :], twist_ref[1, b : b + 1, :]
            work_ref[b, at, :INNER] = re * c - im * s
            work_ref[b, at, INNER:] = im * c + re * s
        return carry

    lax.fori_loop(0, rows // 8, step, 0)
    done = triple_dot(work_ref[...].reshape(outer * rows, 2 * INNER), back_ref)
    out_ref[0] = done[:, :INNER].reshape(outer, rows, INNER)
    out_ref[1] = done[:, INNER:].reshape(outer, rows, INNER)


VMEM = pl.BlockSpec(memory_space=pltpu.VMEM)


def local(chans, slabs, taylor_models, gridded_vis, uv_weight, freq_ratio, robust_scale):
    terms, rows, width = taylor_models.shape
    points = rows * slabs
    outer = points // INNER
    own_a, own_b, own_k = INNER // slabs, outer // chans, INNER // slabs
    ahead, back, twist = (jnp.asarray(t) for t in tables(points))
    f32 = jnp.float32
    offsets = lax.all_gather(freq_ratio, "chan", axis=0, tiled=True) - 1.0
    powers = jnp.stack([offsets**t for t in range(terms)])

    send = taylor_models.reshape(terms, own_a, chans, own_b, width).transpose(2, 0, 3, 1, 4)
    lines = terms * own_b * own_a
    got = lax.all_to_all(
        send.reshape(chans, lines, width), "chan", split_axis=0, concat_axis=0, tiled=True
    )
    part = pl.pallas_call(
        rows_forward,
        out_shape=jax.ShapeDtypeStruct((2, outer, INNER, lines), f32),
        in_specs=[VMEM] * 3,
        out_specs=VMEM,
        name="rows_forward",
    )(got, ahead, twist)

    send = part.reshape(2, outer, slabs, own_k, lines).transpose(2, 0, 1, 3, 4)
    got = lax.all_to_all(send, "slab", split_axis=0, concat_axis=0, tiled=True)
    got = got.reshape(slabs, 2, outer, own_k, terms, own_b, own_a)
    got = got.transpose(4, 1, 5, 3, 2, 0, 6).reshape(terms, 2, own_b, rows, INNER)
    mixed = got[0][None] + sum(
        powers[t][:, None, None, None, None] * got[t][None] for t in range(1, terms)
    )
    got = lax.all_to_all(mixed, "chan", split_axis=0, concat_axis=0, tiled=True)
    full = got.transpose(1, 0, 2, 3, 4).reshape(2, outer, rows, INNER)

    block = min(rows, 64)
    shape = (2, outer, block, INNER)
    result = pl.pallas_call(
        middle,
        grid=(rows // block,),
        out_shape=jax.ShapeDtypeStruct((2, outer, rows, INNER), f32),
        in_specs=[
            pl.BlockSpec(memory_space=pltpu.SMEM),
            pl.BlockSpec(shape, lambda i: (0, 0, i, 0)),
            pl.BlockSpec((1, 2, block, points), lambda i: (0, 0, i, 0)),
            pl.BlockSpec((1, block, points), lambda i: (0, i, 0)),
            pl.BlockSpec((2, 2 * INNER, 2 * INNER), lambda i: (0, 0, 0)),
            pl.BlockSpec((2, 2 * INNER, 2 * INNER), lambda i: (0, 0, 0)),
            pl.BlockSpec((2, outer, INNER), lambda i: (0, 0, 0)),
        ],
        out_specs=pl.BlockSpec(shape, lambda i: (0, 0, i, 0)),
        scratch_shapes=[
            pltpu.VMEM((outer, block, 2 * INNER), f32),
            pltpu.VMEM((3, block, points), f32),
        ],
        name="middle",
    )(robust_scale, full, gridded_vis, uv_weight, ahead, back, twist)

    send = result.reshape(2, chans, own_b, rows, INNER).transpose(1, 0, 2, 3, 4)
    got = lax.all_to_all(send, "chan", split_axis=0, concat_axis=0, tiled=True)
    summed = jnp.stack(
        [sum(powers[t, c] * got[c] for c in range(chans)) for t in range(terms)]
    )
    send = summed.reshape(terms, 2, own_b, own_k, outer, slabs, own_a)
    send = send.transpose(5, 1, 4, 3, 0, 2, 6).reshape(slabs, 2, outer, own_k, lines)
    got = lax.all_to_all(send, "slab", split_axis=0, concat_axis=0, tiled=True)
    part = got.transpose(1, 2, 0, 3, 4).reshape(2, outer, INNER, lines)
    image = pl.pallas_call(
        rows_inverse,
        out_shape=jax.ShapeDtypeStruct((chans, lines, width), f32),
        in_specs=[VMEM] * 3,
        out_specs=VMEM,
        name="rows_inverse",
    )(part, back, twist)
    got = lax.all_to_all(image, "chan", split_axis=0, concat_axis=0, tiled=True)
    got = got.reshape(chans, terms, own_b, own_a, width).transpose(1, 3, 0, 2, 4)
    return got.reshape(terms, rows, width)


def solution(mesh):
    placed = (
        P(None, "slab", "chan"),
        P("chan", None, "slab", None),
        P("chan", "slab", None),
        P("chan"),
        P("chan"),
    )
    body = functools.partial(local, mesh.shape["chan"], mesh.shape["slab"])
    return jax.shard_map(
        body, mesh=mesh, in_specs=placed, out_specs=P(None, "slab", "chan"), check_vma=False
    )
```

```python
import functools
import math

import jax
import jax.numpy as jnp
import numpy as np
from jax import lax
from jax.experimental import pallas as pl
from jax.experimental.pallas import tpu as pltpu
from jax.sharding import PartitionSpec as P

INNER = 128
CHUNKS = 2


def split_bf16(x):
    high = x.astype(jnp.bfloat16)
    low = (x - high.astype(jnp.float32)).astype(jnp.bfloat16)
    return high, low


def table_pair(table):
    high = table.astype(np.float32).astype(jnp.bfloat16)
    low = (table - high.astype(np.float64)).astype(np.float32).astype(jnp.bfloat16)
    return np.stack([high, low])


@functools.cache
def tables(points):
    outer = points // INNER
    steps = np.arange(INNER)
    angle = 2.0 * np.pi * (np.outer(steps, steps) % INNER) / INNER
    cos, sin = np.cos(angle), np.sin(angle)
    forward = np.block([[cos, -sin], [sin, cos]])
    inverse = np.block([[cos, sin], [-sin, cos]])
    twist = 2.0 * np.pi * np.outer(np.arange(outer), steps) / points
    twist_table = np.stack([np.cos(twist), np.sin(twist)]).astype(np.float32)
    return table_pair(forward), table_pair(inverse), twist_table


def plus(x, y):
    return y if x is None else x if y is None else x + y


def minus(x, y):
    if y is None:
        return x
    return -y if x is None else x - y


def short_dft(values, sign):
    count = len(values)
    if count == 1:
        return values
    even = short_dft(values[0::2], sign)
    odd = short_dft(values[1::2], sign)
    half = count // 2
    out = [None] * count
    for k in range(half):
        (er, ei), (orr, oi) = even[k], odd[k]
        if k == 0:
            tr, ti = orr, oi
        elif 4 * k == count:
            tr, ti = (minus(None, oi), orr) if sign > 0 else (oi, minus(None, orr))
        else:
            c = math.cos(2.0 * math.pi * k / count)
            s = sign * math.sin(2.0 * math.pi * k / count)
            tr = minus(orr * c, None if oi is None else oi * s)
            ti = plus(orr * s, None if oi is None else oi * c)
        out[k] = (plus(er, tr), plus(ei, ti))
        out[k + half] = (minus(er, tr), minus(ei, ti))
    return out


def triple_dot(x, table_ref):
    high, low = split_bf16(x)
    dot = functools.partial(jnp.dot, preferred_element_type=jnp.float32)
    return dot(high, table_ref[0]) + dot(low, table_ref[0]) + dot(high, table_ref[1])


def rows_forward(x_ref, table_ref, twist_ref, *out_refs):
    blocks, rows, width = x_ref.shape
    outer = blocks * width // INNER
    pieces = []
    for block in range(blocks):
        for start in range(0, width, INNER):
            pieces.append((x_ref[block, :, start : start + INNER], None))
    parts = short_dft(pieces, -1)
    turned = []
    for j in range(outer):
        re, im = parts[j]
        if im is None:
            im = jnp.zeros_like(re)
        c, s = twist_ref[0, j : j + 1, :], twist_ref[1, j : j + 1, :]
        turned.append(jnp.concatenate([re * c + im * s, im * c - re * s], axis=1))
    done = triple_dot(jnp.concatenate(turned, axis=0), table_ref)
    slabs, _, per_chunk = out_refs[0].shape[:3]
    own_k = per_chunk * len(out_refs)
    for j in range(outer):
        flipped = done[j * rows : (j + 1) * rows].T
        for slab in range(slabs):
            for chunk, out_ref in enumerate(out_refs):
                for part in range(2):
                    start = part * INNER + slab * own_k + chunk * per_chunk
                    out_ref[slab, part, :, j, :] = flipped[start : start + per_chunk]


def rows_inverse(table_ref, twist_ref, *refs):
    x_refs, out_ref = refs[:-1], refs[-1]
    blocks, rows, width = out_ref.shape
    slabs, _, _, outer, _ = x_refs[0].shape
    scale = 1.0 / (outer * INNER)
    lines = []
    for j in range(outer):
        line = [
            x_ref[slab, part, :, j, :]
            for part in range(2)
            for slab in range(slabs)
            for x_ref in x_refs
        ]
        lines.append(jnp.concatenate(line, axis=0).T)
    done = triple_dot(jnp.concatenate(lines, axis=0), table_ref)
    turned = []
    for j in range(outer):
        part = done[j * rows : (j + 1) * rows]
        re, im = part[:, :INNER], part[:, INNER:]
        c, s = twist_ref[0, j : j + 1, :] * scale, twist_ref[1, j : j + 1, :] * scale
        turned.append((re * c - im * s, im * c + re * s))
    result = short_dft(turned, 1)
    per_block = width // INNER
    for b in range(outer):
        start = (b % per_block) * INNER
        out_ref[b // per_block, :, start : start + INNER] = result[b][0]


def mix(power_ref, x_ref, out_ref):
    slabs, _, _, lines = x_ref.shape
    chans, _, own_b, _, _ = out_ref.shape
    terms = power_ref.shape[0]
    own_a = lines // (terms * own_b)
    x = [x_ref[slab, 0] for slab in range(slabs)]
    for b in range(own_b):
        by_term = []
        for t in range(terms):
            start = (t * own_b + b) * own_a
            by_term.append(jnp.concatenate([p[:, start : start + own_a] for p in x], axis=1))
        for c in range(chans):
            total = by_term[0]
            for t in range(1, terms):
                total = total + power_ref[t, c] * by_term[t]
            out_ref[c, 0, b] = total


def gather_terms(power_ref, x_ref, out_ref):
    chans, _, own_b, _, _ = x_ref.shape
    slabs, _, _, lines = out_ref.shape
    terms = power_ref.shape[0]
    own_a = lines // (terms * own_b)
    sums = []
    for t in range(terms):
        for b in range(own_b):
            total = x_ref[0, 0, b] if t == 0 else power_ref[t, 0] * x_ref[0, 0, b]
            for c in range(1, chans):
                total = total + (x_ref[c, 0, b] if t == 0 else power_ref[t, c] * x_ref[c, 0, b])
            sums.append(total)
    for slab in range(slabs):
        lanes = slice(slab * own_a, (slab + 1) * own_a)
        out_ref[slab, 0] = jnp.concatenate([total[:, lanes] for total in sums], axis=1)


def middle(
    damping_ref, x_ref, vis_ref, weight_ref, ahead_ref, back_ref, twist_ref, out_ref, work_ref, wide_ref
):
    chans, _, own_b, rows, _ = x_ref.shape
    outer = chans * own_b
    scale = 1.0 / (outer * INNER)
    joined = jnp.concatenate(
        [x_ref[:, part].reshape(outer * rows, INNER) for part in range(2)], axis=1
    )
    work_ref[...] = triple_dot(joined, ahead_ref).reshape(outer, rows, 2 * INNER)
    wide_ref[0] = vis_ref[0, 0].astype(jnp.float32)
    wide_ref[1] = vis_ref[0, 1].astype(jnp.float32)
    wide_ref[2] = weight_ref[0].astype(jnp.float32)
    damping = damping_ref[0]

    def step(index, carry):
        at = pl.ds(pl.multiple_of(index * 8, 8), 8)
        values = []
        for b in range(outer):
            re, im = work_ref[b, at, :INNER], work_ref[b, at, INNER:]
            c, s = twist_ref[0, b : b + 1, :] * scale, twist_ref[1, b : b + 1, :] * scale
            values.append((re * c + im * s, im * c - re * s))
        spectrum = short_dft(values, -1)
        weighted = []
        for j in range(outer):
            lanes = slice(j * INNER, (j + 1) * INNER)
            weight = wide_ref[2, at, lanes]
            re = wide_ref[0, at, lanes] - weight * spectrum[j][0]
            im = wide_ref[1, at, lanes] - weight * spectrum[j][1]
            robust = 1.0 / (1.0 + damping * (re * re + im * im))
            weighted.append((robust * re, robust * im))
        inverse = short_dft(weighted, 1)
        for b in range(outer):
            re, im = inverse[b]
            c, s = twist_ref[0, b : b + 1, :], twist_ref[1, b : b + 1, :]
            work_ref[b, at, :INNER] = re * c - im * s
            work_ref[b, at, INNER:] = im * c + re * s
        return carry

    lax.fori_loop(0, rows // 8, step, 0)
    done = triple_dot(work_ref[...].reshape(outer * rows, 2 * INNER), back_ref)
    out_ref[:, 0] = done[:, :INNER].reshape(chans, own_b, rows, INNER)
    out_ref[:, 1] = done[:, INNER:].reshape(chans, own_b, rows, INNER)


VMEM = pl.BlockSpec(memory_space=pltpu.VMEM)


def local(chans, slabs, taylor_models, gridded_vis, uv_weight, freq_ratio, robust_scale):
    terms, rows, width = taylor_models.shape
    points = rows * slabs
    outer = points // INNER
    own_a, own_b, own_k = INNER // slabs, outer // chans, INNER // slabs
    ahead, back, twist = (jnp.asarray(t) for t in tables(points))
    f32 = jnp.float32
    offsets = lax.all_gather(freq_ratio, "chan", axis=0, tiled=True) - 1.0
    powers = jnp.stack([offsets**t for t in range(terms)])

    send = taylor_models.reshape(terms, own_a, chans, own_b, width).transpose(2, 0, 3, 1, 4)
    lines = terms * own_b * own_a
    got = lax.all_to_all(
        send.reshape(chans, lines, width), "chan", split_axis=0, concat_axis=0, tiled=True
    )
    chunks = CHUNKS if own_k % CHUNKS == 0 else 1
    own_u = rows // chunks
    parts = pl.pallas_call(
        rows_forward,
        out_shape=[
            jax.ShapeDtypeStruct((slabs, 2, own_k // chunks, outer, lines), f32)
            for _ in range(chunks)
        ],
        in_specs=[VMEM] * 3,
        out_specs=[VMEM] * chunks,
        name="rows_forward",
    )(got, ahead, twist)

    exchange = functools.partial(lax.all_to_all, split_axis=0, concat_axis=0, tiled=True)
    smem = pl.BlockSpec(memory_space=pltpu.SMEM)
    step = min(own_u, 64)
    by_chan = (chans, 2, own_b, own_u, INNER)
    by_slab = (slabs, 2, own_u, lines)
    chan_spec = pl.BlockSpec((chans, 1, own_b, step, INNER), lambda p, i: (0, p, 0, i, 0))
    slab_spec = pl.BlockSpec((slabs, 1, step, lines), lambda p, i: (0, p, i, 0))
    block = min(own_u, 64)
    whole_spec = pl.BlockSpec((chans, 2, own_b, block, INNER), lambda i: (0, 0, 0, i, 0))

    arrived = [exchange(part.reshape(by_slab), "slab") for part in parts]
    full = []
    for got in arrived:
        mixed = pl.pallas_call(
            mix,
            grid=(2, own_u // step),
            out_shape=jax.ShapeDtypeStruct(by_chan, f32),
            in_specs=[smem, slab_spec],
            out_specs=chan_spec,
            name="mix",
        )(powers, got)
        full.append(exchange(mixed, "chan"))

    back_parts = []
    for chunk, got in enumerate(full):
        first = chunk * (own_u // block)
        result = pl.pallas_call(
            middle,
            grid=(own_u // block,),
            out_shape=jax.ShapeDtypeStruct(by_chan, f32),
            in_specs=[
                smem,
                whole_spec,
                pl.BlockSpec((1, 2, block, points), lambda i, first=first: (0, 0, i + first, 0)),
                pl.BlockSpec((1, block, points), lambda i, first=first: (0, i + first, 0)),
                pl.BlockSpec((2, 2 * INNER, 2 * INNER), lambda i: (0, 0, 0)),
                pl.BlockSpec((2, 2 * INNER, 2 * INNER), lambda i: (0, 0, 0)),
                pl.BlockSpec((2, outer, INNER), lambda i: (0, 0, 0)),
            ],
            out_specs=whole_spec,
            scratch_shapes=[
                pltpu.VMEM((outer, block, 2 * INNER), f32),
                pltpu.VMEM((3, block, points), f32),
            ],
            name="middle",
        )(robust_scale, got, gridded_vis, uv_weight, ahead, back, twist)
        got = exchange(result, "chan")
        summed = pl.pallas_call(
            gather_terms,
            grid=(2, own_u // step),
            out_shape=jax.ShapeDtypeStruct(by_slab, f32),
            in_specs=[smem, chan_spec],
            out_specs=slab_spec,
            name="gather_terms",
        )(powers, got)
        got = exchange(summed, "slab")
        back_parts.append(got.reshape(slabs, 2, own_k // chunks, outer, lines))

    image = pl.pallas_call(
        rows_inverse,
        out_shape=jax.ShapeDtypeStruct((chans, lines, width), f32),
        in_specs=[VMEM] * (2 + chunks),
        out_specs=VMEM,
        name="rows_inverse",
    )(back, twist, *back_parts)
    got = lax.all_to_all(image, "chan", split_axis=0, concat_axis=0, tiled=True)
    got = got.reshape(chans, terms, own_b, own_a, width).transpose(1, 3, 0, 2, 4)
    return got.reshape(terms, rows, width)


def solution(mesh):
    placed = (
        P(None, "slab", "chan"),
        P("chan", None, "slab", None),
        P("chan", "slab", None),
        P("chan"),
        P("chan"),
    )
    body = functools.partial(local, mesh.shape["chan"], mesh.shape["slab"])
    return jax.shard_map(
        body, mesh=mesh, in_specs=placed, out_specs=P(None, "slab", "chan"), check_vma=False
    )
```

```python
import functools
import math

import jax
import jax.numpy as jnp
import numpy as np
from jax import lax
from jax.experimental import pallas as pl
from jax.experimental.pallas import tpu as pltpu
from jax.sharding import PartitionSpec as P

INNER = 128
CHUNKS = 2


def split_bf16(x):
    high = x.astype(jnp.bfloat16)
    low = (x - high.astype(jnp.float32)).astype(jnp.bfloat16)
    return high, low


def table_pair(table):
    high = table.astype(np.float32).astype(jnp.bfloat16)
    low = (table - high.astype(np.float64)).astype(np.float32).astype(jnp.bfloat16)
    return np.stack([high, low])


@functools.cache
def tables(points):
    outer = points // INNER
    steps = np.arange(INNER)
    angle = 2.0 * np.pi * (np.outer(steps, steps) % INNER) / INNER
    cos, sin = np.cos(angle), np.sin(angle)
    forward = np.block([[cos, -sin], [sin, cos]])
    inverse = np.block([[cos, sin], [-sin, cos]])
    twist = 2.0 * np.pi * np.outer(np.arange(outer), steps) / points
    twist_table = np.stack([np.cos(twist), np.sin(twist)]).astype(np.float32)
    return table_pair(forward), table_pair(inverse), twist_table


def plus(x, y):
    return y if x is None else x if y is None else x + y


def minus(x, y):
    if y is None:
        return x
    return -y if x is None else x - y


def short_dft(values, sign):
    count = len(values)
    if count == 1:
        return values
    even = short_dft(values[0::2], sign)
    odd = short_dft(values[1::2], sign)
    half = count // 2
    out = [None] * count
    for k in range(half):
        (er, ei), (orr, oi) = even[k], odd[k]
        if k == 0:
            tr, ti = orr, oi
        elif 4 * k == count:
            tr, ti = (minus(None, oi), orr) if sign > 0 else (oi, minus(None, orr))
        else:
            c = math.cos(2.0 * math.pi * k / count)
            s = sign * math.sin(2.0 * math.pi * k / count)
            tr = minus(orr * c, None if oi is None else oi * s)
            ti = plus(orr * s, None if oi is None else oi * c)
        out[k] = (plus(er, tr), plus(ei, ti))
        out[k + half] = (minus(er, tr), minus(ei, ti))
    return out


def triple_dot(x, table_ref):
    high, low = split_bf16(x)
    dot = functools.partial(jnp.dot, preferred_element_type=jnp.float32)
    return dot(high, table_ref[0]) + dot(low, table_ref[0]) + dot(high, table_ref[1])


def rows_forward(x_ref, table_ref, twist_ref, *out_refs):
    blocks, rows, width = x_ref.shape
    outer = blocks * width // INNER
    pieces = []
    for block in range(blocks):
        for start in range(0, width, INNER):
            pieces.append((x_ref[block, :, start : start + INNER], None))
    parts = short_dft(pieces, -1)
    turned = []
    for j in range(outer):
        re, im = parts[j]
        if im is None:
            im = jnp.zeros_like(re)
        c, s = twist_ref[0, j : j + 1, :], twist_ref[1, j : j + 1, :]
        turned.append(jnp.concatenate([re * c + im * s, im * c - re * s], axis=1))
    done = triple_dot(jnp.concatenate(turned, axis=0), table_ref)
    slabs, _, per_chunk = out_refs[0].shape[:3]
    own_k = per_chunk * len(out_refs)
    for j in range(outer):
        flipped = done[j * rows : (j + 1) * rows].T
        for slab in range(slabs):
            for chunk, out_ref in enumerate(out_refs):
                for part in range(2):
                    start = part * INNER + slab * own_k + chunk * per_chunk
                    out_ref[slab, part, :, j, :] = flipped[start : start + per_chunk]


def rows_inverse(table_ref, twist_ref, *refs):
    x_refs, out_ref = refs[:-1], refs[-1]
    blocks, rows, width = out_ref.shape
    slabs, _, _, outer, _ = x_refs[0].shape
    scale = 1.0 / (outer * INNER)
    lines = []
    for j in range(outer):
        line = [
            x_ref[slab, part, :, j, :]
            for part in range(2)
            for slab in range(slabs)
            for x_ref in x_refs
        ]
        lines.append(jnp.concatenate(line, axis=0).T)
    done = triple_dot(jnp.concatenate(lines, axis=0), table_ref)
    turned = []
    for j in range(outer):
        part = done[j * rows : (j + 1) * rows]
        re, im = part[:, :INNER], part[:, INNER:]
        c, s = twist_ref[0, j : j + 1, :] * scale, twist_ref[1, j : j + 1, :] * scale
        turned.append((re * c - im * s, im * c + re * s))
    result = short_dft(turned, 1)
    per_block = width // INNER
    for b in range(outer):
        start = (b % per_block) * INNER
        out_ref[b // per_block, :, start : start + INNER] = result[b][0]


def mix(peer_ref, power_ref, x_ref, *out_refs):
    slabs, _, _, lines = x_ref.shape
    own_b = out_refs[0].shape[1]
    terms = power_ref.shape[0]
    own_a = lines // (terms * own_b)
    x = [x_ref[slab, 0] for slab in range(slabs)]
    for b in range(own_b):
        by_term = []
        for t in range(terms):
            start = (t * own_b + b) * own_a
            by_term.append(jnp.concatenate([p[:, start : start + own_a] for p in x], axis=1))
        for d, out_ref in enumerate(out_refs):
            total = by_term[0]
            for t in range(1, terms):
                total = total + power_ref[t, peer_ref[d]] * by_term[t]
            out_ref[0, b] = total


def gather_terms(peer_ref, power_ref, *refs):
    x_refs, out_ref = refs[:-1], refs[-1]
    own_b = x_refs[0].shape[1]
    slabs, _, _, lines = out_ref.shape
    terms = power_ref.shape[0]
    own_a = lines // (terms * own_b)
    sums = []
    for t in range(terms):
        for b in range(own_b):
            total = None
            for d, x_ref in enumerate(x_refs):
                piece = x_ref[0, b]
                if t:
                    piece = power_ref[t, peer_ref[d]] * piece
                total = piece if total is None else total + piece
            sums.append(total)
    for slab in range(slabs):
        lanes = slice(slab * own_a, (slab + 1) * own_a)
        out_ref[slab, 0] = jnp.concatenate([total[:, lanes] for total in sums], axis=1)


def middle(peer_ref, damping_ref, vis_ref, weight_ref, ahead_ref, back_ref, twist_ref, *refs):
    count = (len(refs) - 2) // 2
    x_refs, out_refs = refs[:count], refs[count : 2 * count]
    work_ref, wide_ref = refs[2 * count :]
    _, own_b, rows, _ = x_refs[0].shape
    outer = count * own_b
    scale = 1.0 / (outer * INNER)
    for d, x_ref in enumerate(x_refs):
        joined = jnp.concatenate(
            [x_ref[part].reshape(own_b * rows, INNER) for part in range(2)], axis=1
        )
        done = triple_dot(joined, ahead_ref).reshape(own_b, rows, 2 * INNER)
        work_ref[pl.ds(peer_ref[d] * own_b, own_b)] = done
    wide_ref[0] = vis_ref[0, 0].astype(jnp.float32)
    wide_ref[1] = vis_ref[0, 1].astype(jnp.float32)
    wide_ref[2] = weight_ref[0].astype(jnp.float32)
    damping = damping_ref[0]

    def step(index, carry):
        at = pl.ds(pl.multiple_of(index * 8, 8), 8)
        values = []
        for b in range(outer):
            re, im = work_ref[b, at, :INNER], work_ref[b, at, INNER:]
            c, s = twist_ref[0, b : b + 1, :] * scale, twist_ref[1, b : b + 1, :] * scale
            values.append((re * c + im * s, im * c - re * s))
        spectrum = short_dft(values, -1)
        weighted = []
        for j in range(outer):
            lanes = slice(j * INNER, (j + 1) * INNER)
            weight = wide_ref[2, at, lanes]
            re = wide_ref[0, at, lanes] - weight * spectrum[j][0]
            im = wide_ref[1, at, lanes] - weight * spectrum[j][1]
            robust = 1.0 / (1.0 + damping * (re * re + im * im))
            weighted.append((robust * re, robust * im))
        inverse = short_dft(weighted, 1)
        for b in range(outer):
            re, im = inverse[b]
            c, s = twist_ref[0, b : b + 1, :], twist_ref[1, b : b + 1, :]
            work_ref[b, at, :INNER] = re * c - im * s
            work_ref[b, at, INNER:] = im * c + re * s
        return carry

    lax.fori_loop(0, rows // 8, step, 0)
    for d, out_ref in enumerate(out_refs):
        lines = work_ref[pl.ds(peer_ref[d] * own_b, own_b)].reshape(own_b * rows, 2 * INNER)
        done = triple_dot(lines, back_ref)
        out_ref[0] = done[:, :INNER].reshape(own_b, rows, INNER)
        out_ref[1] = done[:, INNER:].reshape(own_b, rows, INNER)


def swap(pieces, count):
    out = [pieces[0]]
    for d in range(1, count):
        pairs = [(c, c ^ d) for c in range(count)]
        out.append(lax.ppermute(pieces[d], "chan", pairs))
    return out


VMEM = pl.BlockSpec(memory_space=pltpu.VMEM)


def local(chans, slabs, taylor_models, gridded_vis, uv_weight, freq_ratio, robust_scale):
    terms, rows, width = taylor_models.shape
    points = rows * slabs
    outer = points // INNER
    own_a, own_b, own_k = INNER // slabs, outer // chans, INNER // slabs
    ahead, back, twist = (jnp.asarray(t) for t in tables(points))
    f32 = jnp.float32
    offsets = lax.all_gather(freq_ratio, "chan", axis=0, tiled=True) - 1.0
    powers = jnp.stack([offsets**t for t in range(terms)])

    send = taylor_models.reshape(terms, own_a, chans, own_b, width).transpose(2, 0, 3, 1, 4)
    lines = terms * own_b * own_a
    got = lax.all_to_all(
        send.reshape(chans, lines, width), "chan", split_axis=0, concat_axis=0, tiled=True
    )
    chunks = CHUNKS if own_k % CHUNKS == 0 else 1
    own_u = rows // chunks
    parts = pl.pallas_call(
        rows_forward,
        out_shape=[
            jax.ShapeDtypeStruct((slabs, 2, own_k // chunks, outer, lines), f32)
            for _ in range(chunks)
        ],
        in_specs=[VMEM] * 3,
        out_specs=[VMEM] * chunks,
        name="rows_forward",
    )(got, ahead, twist)

    exchange = functools.partial(lax.all_to_all, split_axis=0, concat_axis=0, tiled=True)
    smem = pl.BlockSpec(memory_space=pltpu.SMEM)
    step = min(own_u, 64)
    peers = lax.axis_index("chan") ^ jnp.arange(chans, dtype=jnp.int32)
    by_peer = [jax.ShapeDtypeStruct((2, own_b, own_u, INNER), f32)] * chans
    by_slab = (slabs, 2, own_u, lines)
    peer_specs = [pl.BlockSpec((1, own_b, step, INNER), lambda p, i: (p, 0, i, 0))] * chans
    slab_spec = pl.BlockSpec((slabs, 1, step, lines), lambda p, i: (0, p, i, 0))
    block = min(own_u, 64)
    whole_specs = [pl.BlockSpec((2, own_b, block, INNER), lambda i: (0, 0, i, 0))] * chans

    arrived = [exchange(part.reshape(by_slab), "slab") for part in parts]
    full = []
    for got in arrived:
        mixed = pl.pallas_call(
            mix,
            grid=(2, own_u // step),
            out_shape=by_peer,
            in_specs=[smem, smem, slab_spec],
            out_specs=peer_specs,
            name="mix",
        )(peers, powers, got)
        full.append(swap(mixed, chans))

    back_parts = []
    for chunk, got in enumerate(full):
        first = chunk * (own_u // block)
        result = pl.pallas_call(
            middle,
            grid=(own_u // block,),
            out_shape=by_peer,
            in_specs=[
                smem,
                smem,
                pl.BlockSpec((1, 2, block, points), lambda i, first=first: (0, 0, i + first, 0)),
                pl.BlockSpec((1, block, points), lambda i, first=first: (0, i + first, 0)),
                pl.BlockSpec((2, 2 * INNER, 2 * INNER), lambda i: (0, 0, 0)),
                pl.BlockSpec((2, 2 * INNER, 2 * INNER), lambda i: (0, 0, 0)),
                pl.BlockSpec((2, outer, INNER), lambda i: (0, 0, 0)),
                *whole_specs,
            ],
            out_specs=whole_specs,
            scratch_shapes=[
                pltpu.VMEM((outer, block, 2 * INNER), f32),
                pltpu.VMEM((3, block, points), f32),
            ],
            name="middle",
        )(peers, robust_scale, gridded_vis, uv_weight, ahead, back, twist, *got)
        got = swap(result, chans)
        summed = pl.pallas_call(
            gather_terms,
            grid=(2, own_u // step),
            out_shape=jax.ShapeDtypeStruct(by_slab, f32),
            in_specs=[smem, smem, *peer_specs],
            out_specs=slab_spec,
            name="gather_terms",
        )(peers, powers, *got)
        got = exchange(summed, "slab")
        back_parts.append(got.reshape(slabs, 2, own_k // chunks, outer, lines))

    image = pl.pallas_call(
        rows_inverse,
        out_shape=jax.ShapeDtypeStruct((chans, lines, width), f32),
        in_specs=[VMEM] * (2 + chunks),
        out_specs=VMEM,
        name="rows_inverse",
    )(back, twist, *back_parts)
    got = lax.all_to_all(image, "chan", split_axis=0, concat_axis=0, tiled=True)
    got = got.reshape(chans, terms, own_b, own_a, width).transpose(1, 3, 0, 2, 4)
    return got.reshape(terms, rows, width)


def solution(mesh):
    placed = (
        P(None, "slab", "chan"),
        P("chan", None, "slab", None),
        P("chan", "slab", None),
        P("chan"),
        P("chan"),
    )
    body = functools.partial(local, mesh.shape["chan"], mesh.shape["slab"])
    return jax.shard_map(
        body, mesh=mesh, in_specs=placed, out_specs=P(None, "slab", "chan"), check_vma=False
    )
```

```python
import functools
import math

import jax
import jax.numpy as jnp
import numpy as np
from jax import lax
from jax.experimental import pallas as pl
from jax.experimental.pallas import tpu as pltpu
from jax.sharding import PartitionSpec as P

INNER = 128
CHUNKS = 2


def split_bf16(x):
    high = x.astype(jnp.bfloat16)
    low = (x - high.astype(jnp.float32)).astype(jnp.bfloat16)
    return high, low


def table_pair(table):
    high = table.astype(np.float32).astype(jnp.bfloat16)
    low = (table - high.astype(np.float64)).astype(np.float32).astype(jnp.bfloat16)
    return np.stack([high, low])


@functools.cache
def tables(points):
    outer = points // INNER
    steps = np.arange(INNER)
    angle = 2.0 * np.pi * (np.outer(steps, steps) % INNER) / INNER
    cos, sin = np.cos(angle), np.sin(angle)
    forward = np.block([[cos, -sin], [sin, cos]])
    inverse = np.block([[cos, sin], [-sin, cos]])
    twist = 2.0 * np.pi * np.outer(np.arange(outer), steps) / points
    twist_table = np.stack([np.cos(twist), np.sin(twist)]).astype(np.float32)
    return table_pair(forward), table_pair(inverse), twist_table


def plus(x, y):
    return y if x is None else x if y is None else x + y


def minus(x, y):
    if y is None:
        return x
    return -y if x is None else x - y


def short_dft(values, sign):
    count = len(values)
    if count == 1:
        return values
    even = short_dft(values[0::2], sign)
    odd = short_dft(values[1::2], sign)
    half = count // 2
    out = [None] * count
    for k in range(half):
        (er, ei), (orr, oi) = even[k], odd[k]
        if k == 0:
            tr, ti = orr, oi
        elif 4 * k == count:
            tr, ti = (minus(None, oi), orr) if sign > 0 else (oi, minus(None, orr))
        else:
            c = math.cos(2.0 * math.pi * k / count)
            s = sign * math.sin(2.0 * math.pi * k / count)
            tr = minus(orr * c, None if oi is None else oi * s)
            ti = plus(orr * s, None if oi is None else oi * c)
        out[k] = (plus(er, tr), plus(ei, ti))
        out[k + half] = (minus(er, tr), minus(ei, ti))
    return out


def triple_dot(x, table_ref):
    high, low = split_bf16(x)
    dot = functools.partial(jnp.dot, preferred_element_type=jnp.float32)
    return dot(high, table_ref[0]) + dot(low, table_ref[0]) + dot(high, table_ref[1])


def rows_forward(x_ref, table_ref, twist_ref, *out_refs):
    blocks, rows, width = x_ref.shape
    outer = blocks * width // INNER
    pieces = []
    for block in range(blocks):
        for start in range(0, width, INNER):
            pieces.append((x_ref[block, :, start : start + INNER], None))
    parts = short_dft(pieces, -1)
    turned = []
    for j in range(outer):
        re, im = parts[j]
        if im is None:
            im = jnp.zeros_like(re)
        c, s = twist_ref[0, j : j + 1, :], twist_ref[1, j : j + 1, :]
        turned.append(jnp.concatenate([re * c + im * s, im * c - re * s], axis=1))
    done = triple_dot(jnp.concatenate(turned, axis=0), table_ref)
    slabs, _, per_chunk = out_refs[0].shape[:3]
    own_k = per_chunk * len(out_refs)
    for j in range(outer):
        flipped = done[j * rows : (j + 1) * rows].T
        for slab in range(slabs):
            for chunk, out_ref in enumerate(out_refs):
                for part in range(2):
                    start = part * INNER + slab * own_k + chunk * per_chunk
                    out_ref[slab, part, :, j, :] = flipped[start : start + per_chunk]


def rows_inverse(table_ref, twist_ref, *refs):
    x_refs, out_ref = refs[:-1], refs[-1]
    blocks, rows, width = out_ref.shape
    slabs, _, _, outer, _ = x_refs[0].shape
    scale = 1.0 / (outer * INNER)
    lines = []
    for j in range(outer):
        line = [
            x_ref[slab, part, :, j, :]
            for part in range(2)
            for slab in range(slabs)
            for x_ref in x_refs
        ]
        lines.append(jnp.concatenate(line, axis=0).T)
    done = triple_dot(jnp.concatenate(lines, axis=0), table_ref)
    turned = []
    for j in range(outer):
        part = done[j * rows : (j + 1) * rows]
        re, im = part[:, :INNER], part[:, INNER:]
        c, s = twist_ref[0, j : j + 1, :] * scale, twist_ref[1, j : j + 1, :] * scale
        turned.append((re * c - im * s, im * c + re * s))
    result = short_dft(turned, 1)
    per_block = width // INNER
    for b in range(outer):
        start = (b % per_block) * INNER
        out_ref[b // per_block, :, start : start + INNER] = result[b][0]


def mix(peer_ref, power_ref, x_ref, *out_refs):
    slabs, _, _, lines = x_ref.shape
    own_b = out_refs[0].shape[1]
    terms = power_ref.shape[0]
    own_a = lines // (terms * own_b)
    x = [x_ref[slab, 0] for slab in range(slabs)]
    for b in range(own_b):
        by_term = []
        for t in range(terms):
            start = (t * own_b + b) * own_a
            by_term.append(jnp.concatenate([p[:, start : start + own_a] for p in x], axis=1))
        for d, out_ref in enumerate(out_refs):
            total = by_term[0]
            for t in range(1, terms):
                total = total + power_ref[t, d] * by_term[t]
            out_ref[0, b] = total


def gather_terms(peer_ref, power_ref, *refs):
    x_refs, out_ref = refs[:-1], refs[-1]
    own_b = x_refs[0].shape[1]
    slabs, _, _, lines = out_ref.shape
    terms = power_ref.shape[0]
    own_a = lines // (terms * own_b)
    sums = []
    for t in range(terms):
        for b in range(own_b):
            total = None
            for d, x_ref in enumerate(x_refs):
                piece = x_ref[0, b]
                if t:
                    piece = power_ref[t, d] * piece
                total = piece if total is None else total + piece
            sums.append(total)
    for slab in range(slabs):
        lanes = slice(slab * own_a, (slab + 1) * own_a)
        out_ref[slab, 0] = jnp.concatenate([total[:, lanes] for total in sums], axis=1)


def middle(peer_ref, damping_ref, vis_ref, weight_ref, ahead_ref, back_ref, twist_ref, *refs):
    count = (len(refs) - 2) // 2
    x_refs, out_refs = refs[:count], refs[count : 2 * count]
    work_ref, wide_ref = refs[2 * count :]
    _, own_b, rows, _ = x_refs[0].shape
    outer = count * own_b
    scale = 1.0 / (outer * INNER)
    for d, x_ref in enumerate(x_refs):
        joined = jnp.concatenate(
            [x_ref[part].reshape(own_b * rows, INNER) for part in range(2)], axis=1
        )
        done = triple_dot(joined, ahead_ref).reshape(own_b, rows, 2 * INNER)
        work_ref[pl.ds(peer_ref[d] * own_b, own_b)] = done
    wide_ref[0] = vis_ref[0, 0].astype(jnp.float32)
    wide_ref[1] = vis_ref[0, 1].astype(jnp.float32)
    wide_ref[2] = weight_ref[0].astype(jnp.float32)
    damping = damping_ref[0]

    def step(index, carry):
        at = pl.ds(pl.multiple_of(index * 8, 8), 8)
        values = []
        for b in range(outer):
            re, im = work_ref[b, at, :INNER], work_ref[b, at, INNER:]
            c, s = twist_ref[0, b : b + 1, :] * scale, twist_ref[1, b : b + 1, :] * scale
            values.append((re * c + im * s, im * c - re * s))
        spectrum = short_dft(values, -1)
        weighted = []
        for j in range(outer):
            lanes = slice(j * INNER, (j + 1) * INNER)
            weight = wide_ref[2, at, lanes]
            re = wide_ref[0, at, lanes] - weight * spectrum[j][0]
            im = wide_ref[1, at, lanes] - weight * spectrum[j][1]
            robust = 1.0 / (1.0 + damping * (re * re + im * im))
            weighted.append((robust * re, robust * im))
        inverse = short_dft(weighted, 1)
        for b in range(outer):
            re, im = inverse[b]
            c, s = twist_ref[0, b : b + 1, :], twist_ref[1, b : b + 1, :]
            work_ref[b, at, :INNER] = re * c - im * s
            work_ref[b, at, INNER:] = im * c + re * s
        return carry

    lax.fori_loop(0, rows // 8, step, 0)
    for d, out_ref in enumerate(out_refs):
        lines = work_ref[pl.ds(peer_ref[d] * own_b, own_b)].reshape(own_b * rows, 2 * INNER)
        done = triple_dot(lines, back_ref)
        out_ref[0] = done[:, :INNER].reshape(own_b, rows, INNER)
        out_ref[1] = done[:, INNER:].reshape(own_b, rows, INNER)


def swap(pieces, count):
    out = [pieces[0]]
    for d in range(1, count):
        pairs = [(c, c ^ d) for c in range(count)]
        out.append(lax.ppermute(pieces[d], "chan", pairs))
    return out


VMEM = pl.BlockSpec(memory_space=pltpu.VMEM)


def local(chans, slabs, taylor_models, gridded_vis, uv_weight, freq_ratio, robust_scale):
    terms, rows, width = taylor_models.shape
    points = rows * slabs
    outer = points // INNER
    own_a, own_b, own_k = INNER // slabs, outer // chans, INNER // slabs
    ahead, back, twist = (jnp.asarray(t) for t in tables(points))
    f32 = jnp.float32
    offsets = jnp.concatenate(swap([freq_ratio] * chans, chans)) - 1.0
    powers = jnp.stack([offsets**t for t in range(terms)])

    send = taylor_models.reshape(terms, own_a, chans, own_b, width).transpose(2, 0, 3, 1, 4)
    lines = terms * own_b * own_a
    got = lax.all_to_all(
        send.reshape(chans, lines, width), "chan", split_axis=0, concat_axis=0, tiled=True
    )
    chunks = CHUNKS if own_k % CHUNKS == 0 else 1
    own_u = rows // chunks
    parts = pl.pallas_call(
        rows_forward,
        out_shape=[
            jax.ShapeDtypeStruct((slabs, 2, own_k // chunks, outer, lines), f32)
            for _ in range(chunks)
        ],
        in_specs=[VMEM] * 3,
        out_specs=[VMEM] * chunks,
        name="rows_forward",
    )(got, ahead, twist)

    exchange = functools.partial(lax.all_to_all, split_axis=0, concat_axis=0, tiled=True)
    smem = pl.BlockSpec(memory_space=pltpu.SMEM)
    step = min(own_u, 64)
    peers = lax.axis_index("chan") ^ jnp.arange(chans, dtype=jnp.int32)
    by_peer = [jax.ShapeDtypeStruct((2, own_b, own_u, INNER), f32)] * chans
    by_slab = (slabs, 2, own_u, lines)
    peer_specs = [pl.BlockSpec((1, own_b, step, INNER), lambda p, i: (p, 0, i, 0))] * chans
    slab_spec = pl.BlockSpec((slabs, 1, step, lines), lambda p, i: (0, p, i, 0))
    block = min(own_u, 64)
    whole_specs = [pl.BlockSpec((2, own_b, block, INNER), lambda i: (0, 0, i, 0))] * chans

    arrived = [exchange(part.reshape(by_slab), "slab") for part in parts]
    full = []
    for got in arrived:
        mixed = pl.pallas_call(
            mix,
            grid=(2, own_u // step),
            out_shape=by_peer,
            in_specs=[smem, smem, slab_spec],
            out_specs=peer_specs,
            name="mix",
        )(peers, powers, got)
        if full:
            full[-1], mixed = lax.optimization_barrier((full[-1], mixed))
        full.append(swap(mixed, chans))

    back_parts, swapped = [], []
    for chunk, got in enumerate(full):
        first = chunk * (own_u // block)
        result = pl.pallas_call(
            middle,
            grid=(own_u // block,),
            out_shape=by_peer,
            in_specs=[
                smem,
                smem,
                pl.BlockSpec((1, 2, block, points), lambda i, first=first: (0, 0, i + first, 0)),
                pl.BlockSpec((1, block, points), lambda i, first=first: (0, i + first, 0)),
                pl.BlockSpec((2, 2 * INNER, 2 * INNER), lambda i: (0, 0, 0)),
                pl.BlockSpec((2, 2 * INNER, 2 * INNER), lambda i: (0, 0, 0)),
                pl.BlockSpec((2, outer, INNER), lambda i: (0, 0, 0)),
                *whole_specs,
            ],
            out_specs=whole_specs,
            scratch_shapes=[
                pltpu.VMEM((outer, block, 2 * INNER), f32),
                pltpu.VMEM((3, block, points), f32),
            ],
            name="middle",
        )(peers, robust_scale, gridded_vis, uv_weight, ahead, back, twist, *got)
        if swapped:
            swapped[-1], result = lax.optimization_barrier((swapped[-1], result))
        swapped.append(swap(result, chans))

    for got in swapped:
        summed = pl.pallas_call(
            gather_terms,
            grid=(2, own_u // step),
            out_shape=jax.ShapeDtypeStruct(by_slab, f32),
            in_specs=[smem, smem, *peer_specs],
            out_specs=slab_spec,
            name="gather_terms",
        )(peers, powers, *got)
        got = exchange(summed, "slab")
        back_parts.append(got.reshape(slabs, 2, own_k // chunks, outer, lines))

    image = pl.pallas_call(
        rows_inverse,
        out_shape=jax.ShapeDtypeStruct((chans, lines, width), f32),
        in_specs=[VMEM] * (2 + chunks),
        out_specs=VMEM,
        name="rows_inverse",
    )(back, twist, *back_parts)
    got = lax.all_to_all(image, "chan", split_axis=0, concat_axis=0, tiled=True)
    got = got.reshape(chans, terms, own_b, own_a, width).transpose(1, 3, 0, 2, 4)
    return got.reshape(terms, rows, width)


def solution(mesh):
    placed = (
        P(None, "slab", "chan"),
        P("chan", None, "slab", None),
        P("chan", "slab", None),
        P("chan"),
        P("chan"),
    )
    body = functools.partial(local, mesh.shape["chan"], mesh.shape["slab"])
    return jax.shard_map(
        body, mesh=mesh, in_specs=placed, out_specs=P(None, "slab", "chan"), check_vma=False
    )
```
